32 devices in a mesh: section: 8 (over z, core), sp: 4 (over y, x).
Axes of the slice: x: 2, y: 2, z: 4, core: 2. Of those that a mesh axis runs over, the one named last changes fastest.
Arguments:
- query: bfloat16 [8, 512, 8192], P('section', 'sp'), may hold values from -11 to 11
- keyval: bfloat16 [8, 512, 2048], P('section', 'sp'), may hold values from -11 to 11
- cache: bfloat16 [8, 8, 256, 256], P('section', 'sp'), may hold values from -4 to 4, as said below
- offsets: int32 [8], P('section'), may hold values from 0 to 8191
- lengths: int32 [8], P('section'), may hold values from 1 to 256
Outputs:
- forwarded: bfloat16 [8, 512, 8192], P('section', 'sp')
The draws below stay inside these ranges and needn't reach their ends.
Inputs may be any that keep to these rules, and one draw needn't show every extreme that they name: `cache`: slot k holds key-value head k * 1; slots that hold the same head are equal.
All inputs are finite; a program needn't handle non-finite values.
Results may differ from the reference program's by a relative error of at most 0.0096.
Values may be sent and summed in bfloat16 or wider, within the bound.
No kernel may reach another device: no remote copies, remote signals or barrier semaphores. Data moves between devices by JAX's collectives and lax.ppermute only.
A program may use at most 64 MiB of HBM per device.

```python
import math
import jax
import jax.numpy as jnp
from jax import lax

QUERY_HEADS = 64
KEY_VALUE_HEADS = 8
HEAD_SIZE = 128
CACHE_POSITIONS = 256
RELAY_SECTIONS = 8
PREFILL_TOKENS = 512
KEY_VALUE_SLOTS = 8
BLOCK = 512


def draw_query(key, part):
    section_key = jax.random.fold_in(key, 11)
    value_entries = jnp.clip(jax.random.normal(section_key, (RELAY_SECTIONS, PREFILL_TOKENS, QUERY_HEADS, HEAD_SIZE), jnp.float32), -4.0, 4.0)
    return value_entries.reshape(RELAY_SECTIONS, PREFILL_TOKENS, QUERY_HEADS * HEAD_SIZE).astype(jnp.bfloat16)


def draw_keyval(key, part):
    section_key = jax.random.fold_in(key, 22)
    value_entries = jnp.clip(jax.random.normal(section_key, (RELAY_SECTIONS, PREFILL_TOKENS, KEY_VALUE_HEADS, 2 * HEAD_SIZE), jnp.float32), -4.0, 4.0)
    return value_entries.reshape(RELAY_SECTIONS, PREFILL_TOKENS, KEY_VALUE_HEADS * 2 * HEAD_SIZE).astype(jnp.bfloat16)


def draw_cache(key, part):
    section_key = jax.random.fold_in(key, 33)
    head_list = jnp.clip(jax.random.normal(section_key, (RELAY_SECTIONS, KEY_VALUE_HEADS, CACHE_POSITIONS, 2 * HEAD_SIZE), jnp.float32), -4.0, 4.0)
    owner_section = jnp.arange(KEY_VALUE_SLOTS, dtype=jnp.int32) * KEY_VALUE_HEADS // KEY_VALUE_SLOTS
    return jnp.take(head_list, owner_section, axis=1).astype(jnp.bfloat16)


def touch_ends(entries, rng, least, top_value):
    dims = entries.shape
    spot = [jax.random.randint(jax.random.fold_in(rng, axis), (), 0, dims[axis]) for axis in range(len(dims))]
    entries = entries.at[tuple(spot)].set(least)
    longest = dims.index(max(dims))
    spot[longest] = (spot[longest] + 1) % dims[longest]
    return entries.at[tuple(spot)].set(top_value)


def setup_inputs(seed: int = 0) -> dict:
    seeds = jax.random.split(jax.random.key(seed), 6)
    query = draw_query(jax.random.fold_in(seeds[5], 71), 0)
    keyval = draw_keyval(jax.random.fold_in(seeds[5], 71), 0)
    cache = draw_cache(jax.random.fold_in(seeds[5], 71), 0)
    offsets = touch_ends(jax.random.randint(seeds[3], (RELAY_SECTIONS,), 0, 16 * PREFILL_TOKENS), jax.random.fold_in(seeds[3], 1), 0, (16 * PREFILL_TOKENS) - 1).astype(jnp.int32)
    lengths = touch_ends(jax.random.randint(seeds[4], (RELAY_SECTIONS,), 1, CACHE_POSITIONS + 1), jax.random.fold_in(seeds[4], 1), 1, CACHE_POSITIONS).astype(jnp.int32)
    return {"query": query, "keyval": keyval, "cache": cache, "offsets": offsets, "lengths": lengths}


ROPE_BASE = 500000.0

def rotation_tables(positions, head_width):
    half_width = head_width // 2
    exponent = jnp.arange(half_width, dtype=jnp.float32) * (-2.0 / head_width)
    frequency = jnp.power(jnp.float32(ROPE_BASE), exponent)
    angle = positions.astype(jnp.float32)[:, None] * frequency[None, :]
    return (jnp.cos(angle), jnp.sin(angle))

def rotate_pair(value_entries, cosine, sine):
    half_width = value_entries.shape[-1] // 2
    first = value_entries[..., :half_width].astype(jnp.float32)
    second = value_entries[..., half_width:].astype(jnp.float32)
    cos_wide = cosine[:, None, :]
    sin_wide = sine[:, None, :]
    return jnp.concatenate([first * cos_wide - second * sin_wide, second * cos_wide + first * sin_wide], axis=-1)

def attend_head(query_rows, key_rows, value_rows, cache_keys, cache_values, length, block_rows):
    scale = 1.0 / math.sqrt(query_rows.shape[-1])
    contract = (((1,), (1,)), ((), ()))
    cache_live = jnp.arange(cache_keys.shape[0], dtype=jnp.int32) < length
    results = []
    for block_index in range(query_rows.shape[0] // block_rows):
        first_row = block_index * block_rows
        key_reach = first_row + block_rows
        block_queries = query_rows[first_row:key_reach]
        cache_scores = lax.dot_general(block_queries, cache_keys, contract, preferred_element_type=jnp.float32) * scale
        own_scores = lax.dot_general(block_queries, key_rows[:key_reach], contract, preferred_element_type=jnp.float32) * scale
        cache_scores = jnp.where(cache_live[None, :], cache_scores, -jnp.inf)
        row_place = first_row + jnp.arange(block_rows, dtype=jnp.int32)
        causal = jnp.arange(key_reach, dtype=jnp.int32)[None, :] <= row_place[:, None]
        own_scores = jnp.where(causal, own_scores, -jnp.inf)
        row_top = jnp.maximum(lax.optimization_barrier(jnp.max(cache_scores, axis=1)), lax.optimization_barrier(jnp.max(own_scores, axis=1)))
        cache_weights = jnp.exp(cache_scores - row_top[:, None])
        own_weights = jnp.exp(own_scores - row_top[:, None])
        row_total = lax.optimization_barrier(jnp.sum(cache_weights, axis=1)) + lax.optimization_barrier(jnp.sum(own_weights, axis=1))
        numerator = jnp.dot(cache_weights.astype(jnp.bfloat16), cache_values, preferred_element_type=jnp.float32)
        numerator = numerator + jnp.dot(own_weights.astype(jnp.bfloat16), value_rows[:key_reach], preferred_element_type=jnp.float32)
        results.append((numerator / row_total[:, None]).astype(jnp.bfloat16))
    return jnp.concatenate(results, axis=0)

def reference(query, keyval, cache, offsets, lengths):
    group_width = QUERY_HEADS // KEY_VALUE_HEADS

    def one_section(items):
        section_query, section_key_value, section_cache, section_offset, section_length = items
        positions = section_offset + jnp.arange(PREFILL_TOKENS, dtype=jnp.int32)
        cosine, sine = rotation_tables(positions, HEAD_SIZE)
        rotated_queries = rotate_pair(section_query.reshape(PREFILL_TOKENS, QUERY_HEADS, HEAD_SIZE), cosine, sine).astype(jnp.bfloat16)
        pair_matched = section_key_value.reshape(PREFILL_TOKENS, KEY_VALUE_HEADS, 2 * HEAD_SIZE)
        rotated_keys = rotate_pair(pair_matched[..., :HEAD_SIZE], cosine, sine).astype(jnp.bfloat16)
        plain_values = pair_matched[..., HEAD_SIZE:]

        def one_head(head_index):
            group_index = head_index // group_width
            slot_index = head_index * KEY_VALUE_SLOTS // QUERY_HEADS
            head_queries = lax.dynamic_index_in_dim(rotated_queries, head_index, 1, False)
            head_keys = lax.dynamic_index_in_dim(rotated_keys, group_index, 1, False)
            head_values = lax.dynamic_index_in_dim(plain_values, group_index, 1, False)
            slot_cache = lax.dynamic_index_in_dim(section_cache, slot_index, 0, False)
            return attend_head(head_queries, head_keys, head_values, slot_cache[:, :HEAD_SIZE], slot_cache[:, HEAD_SIZE:], section_length, BLOCK)
        head_list = lax.map(one_head, jnp.arange(QUERY_HEADS, dtype=jnp.int32))
        return jnp.transpose(head_list, (1, 0, 2)).reshape(PREFILL_TOKENS, QUERY_HEADS * HEAD_SIZE)
    attended = lax.map(one_section, (query, keyval, cache, offsets, lengths))
    return jnp.roll(attended, 1, axis=0)
```

```python
import math

import jax
import jax.numpy as jnp
from jax import lax
from jax.experimental import pallas as pl
from jax.experimental.pallas import tpu as pltpu
from jax.sharding import PartitionSpec as P


QUERY_HEADS = 64
KEY_VALUE_HEADS = 8
HEAD_SIZE = 128
GROUP = QUERY_HEADS // KEY_VALUE_HEADS


ROPE_BASE = 500000.0
MASKED = -1e30
FACTOR = math.log2(math.e) / math.sqrt(HEAD_SIZE)
SPECS = (
    P("section", "sp", None),
    P("section", "sp", None),
    P("section", "sp", None, None),
    P("section"),
    P("section"),
)
VMEM = pl.BlockSpec(memory_space=pltpu.VMEM)
LIMIT = pltpu.CompilerParams(vmem_limit_bytes=20 * 2**20)


def section_shift(value):
    count = lax.axis_size("section")
    return lax.ppermute(value, "section", [(i, (i + 1) % count) for i in range(count)])


def partner_swap(value, bits):
    count = lax.axis_size("sp")
    return lax.ppermute(value, "sp", [(i, i ^ bits) for i in range(count)])


def rotation_tables(positions, head_width):
    half_width = head_width // 2
    exponent = jnp.arange(half_width, dtype=jnp.float32) * (-2.0 / head_width)
    frequency = jnp.power(jnp.float32(ROPE_BASE), exponent)
    angle = positions.astype(jnp.float32)[:, None] * frequency[None, :]
    return (jnp.cos(angle), jnp.sin(angle))


def rotated(value, cosine, sine):
    wide = value.astype(jnp.float32)
    turned = pltpu.roll(wide, HEAD_SIZE // 2, 1)
    return (wide * cosine + turned * sine).astype(jnp.bfloat16)


def pack_kernel(keyval, cache, cosine, sine, length, *packs):
    rows = keyval.shape[0]
    cos_here, sin_here = cosine[...], sine[...]
    positions = cache.shape[1]
    live = length[0].astype(jnp.float32)
    for chunk, pack in enumerate(packs):
        heads = KEY_VALUE_HEADS // len(packs)
        for index in range(heads):
            head = index * len(packs) + chunk
            start = index * rows + (positions if index >= heads // 2 else 0)
            column = head * 2 * HEAD_SIZE
            pack[start : start + rows, :HEAD_SIZE] = rotated(
                keyval[:, column : column + HEAD_SIZE], cos_here, sin_here
            )
            pack[start : start + rows, HEAD_SIZE:] = keyval[
                :, column + HEAD_SIZE : column + 2 * HEAD_SIZE
            ]
        middle = heads // 2 * rows
        pack[middle : middle + positions, :] = cache[chunk]
        last = heads * rows + positions
        pack[last:, :] = jnp.full((pack.shape[0] - last, pack.shape[1]), live, jnp.float32).astype(
            jnp.bfloat16
        )


def turn_kernel(query, cosine, sine, *turned):
    rows = query.shape[0]
    cos_here, sin_here = cosine[...], sine[...]
    for head in range(QUERY_HEADS):
        pair = head // GROUP
        chunk, index = pair % len(turned), pair // len(turned)
        start = (index * GROUP + head % GROUP) * rows
        turned[chunk][start : start + rows, :] = rotated(
            query[:, head * HEAD_SIZE : (head + 1) * HEAD_SIZE], cos_here, sin_here
        )


STEP_HEADS = GROUP


def dot_scores(picked, keys):
    return lax.dot_general(
        picked, keys, (((1,), (1,)), ((), ())), preferred_element_type=jnp.float32
    )


def weighted(weights, values):
    values = jnp.concatenate([values, jnp.ones_like(values)], axis=1)
    return jnp.dot(weights, values, preferred_element_type=jnp.float32)


def live_mask(own, positions):
    last = own.shape[0] - 16
    length = own[last : last + 1, :].astype(jnp.float32)
    place = lax.broadcasted_iota(jnp.int32, (1, positions), 1).astype(jnp.float32)
    return place < length[:, :positions]


def near_kernel(query, own, beside, above, top_ref, sums_ref):
    me = lax.axis_index("sp")
    total = query.shape[0]
    rows = 128
    heads = total // (GROUP * rows)
    positions = own.shape[0] - 16 - heads * rows
    middle = heads // 2 * rows
    blocks = (own, beside, above)
    live = live_mask(own, positions)
    step_rows = STEP_HEADS * rows
    causal = lax.broadcasted_iota(jnp.int32, (rows, rows), 1) <= lax.broadcasted_iota(
        jnp.int32, (rows, rows), 0
    )
    causal = jnp.concatenate([causal] * STEP_HEADS, axis=0)
    for offset in range(len(blocks) + 1):
        head = me ^ offset
        start = pl.multiple_of(head * rows + jnp.where(head >= heads // 2, positions, 0), rows)
        stored = [block[pl.ds(start, rows), :] for block in blocks]
        if offset < len(blocks):
            stored.append(blocks[offset][middle : middle + positions, :])
        keys = jnp.concatenate([part[:, :HEAD_SIZE] for part in stored], axis=0)
        values = jnp.concatenate([part[:, HEAD_SIZE:] for part in stored], axis=0)
        base = pl.multiple_of(head * (GROUP * rows), rows)
        for step in range(GROUP // STEP_HEADS):
            place = pl.ds(base + step * step_rows, step_rows)
            scores = dot_scores(query[place, :], keys)
            parts = [jnp.where(causal, scores[:, :rows], MASKED)]
            for other in range(1, len(blocks)):
                piece = scores[:, other * rows : (other + 1) * rows]
                parts.append(jnp.where((me ^ other) < me, piece, MASKED))
            if offset < len(blocks):
                parts.append(jnp.where(live, scores[:, len(blocks) * rows :], MASKED))
            scores = jnp.concatenate(parts, axis=1)
            top = jnp.max(scores, axis=1, keepdims=True)
            weights = jnp.exp2((scores - top) * FACTOR).astype(jnp.bfloat16)
            sums_ref[place, :] = weighted(weights, values)
            top_ref[place, :] = jnp.broadcast_to(top, (step_rows, HEAD_SIZE))


def far_kernel(query, own, first_half, second_half, top_ref, sums_ref, *rest):
    passed, out, across = rest if len(rest) == 3 else (None, *rest)
    me = lax.axis_index("sp")
    rows = out.shape[0]
    heads = query.shape[0] // (GROUP * rows)
    half = first_half.shape[0]
    positions = 2 * half - heads * rows
    middle = heads // 2 * rows
    width = GROUP * HEAD_SIZE
    across[:half, :] = first_half[...]
    across[half:, :] = second_half[...]
    live = live_mask(own, positions)
    step_rows = STEP_HEADS * rows
    far = heads - 1
    if passed is not None:
        for index in range(heads):
            out[:, 2 * index * width : (2 * index + 1) * width] = passed[
                :, index * width : (index + 1) * width
            ]
    for offset in range(heads):
        head = me ^ offset
        start = pl.multiple_of(head * rows + jnp.where(head >= heads // 2, positions, 0), rows)
        stored = [across[pl.ds(start, rows), :]]
        if offset == far:
            stored.append(across[middle : middle + positions, :])
        keys = jnp.concatenate([part[:, :HEAD_SIZE] for part in stored], axis=0)
        values = jnp.concatenate([part[:, HEAD_SIZE:] for part in stored], axis=0)
        base = pl.multiple_of(head * (GROUP * rows), rows)
        for step in range(GROUP // STEP_HEADS):
            place = pl.ds(base + step * step_rows, step_rows)
            scores = dot_scores(query[place, :], keys)
            parts = [jnp.where((me ^ far) < me, scores[:, :rows], MASKED)]
            if offset == far:
                parts.append(jnp.where(live, scores[:, rows:], MASKED))
            scores = jnp.concatenate(parts, axis=1)
            before = top_ref[place, :]
            top = jnp.maximum(jnp.max(scores, axis=1, keepdims=True), before)
            kept = jnp.exp2((before - top) * FACTOR)
            weights = jnp.exp2(
                (scores - jnp.concatenate([top] * len(parts[:1] + parts[1:] * 2), axis=1)) * FACTOR
            ).astype(jnp.bfloat16)
            sums = weighted(weights, values) + sums_ref[place, :] * jnp.concatenate(
                [kept, kept], axis=1
            )
            result = (sums[:, :HEAD_SIZE] / sums[:, HEAD_SIZE:]).astype(jnp.bfloat16)
            for part in range(STEP_HEADS):
                lane = (step * STEP_HEADS + part) * HEAD_SIZE
                if passed is None:
                    column = head * width + lane
                else:
                    column = (2 * head + 1) * width + lane
                out[:, pl.ds(pl.multiple_of(column, HEAD_SIZE), HEAD_SIZE)] = result[
                    part * rows : (part + 1) * rows
                ]


def near(turned, own, beside, above):
    work = turned.shape[0] * 576
    return pl.pallas_call(
        near_kernel,
        out_shape=[
            jax.ShapeDtypeStruct((turned.shape[0], HEAD_SIZE), jnp.float32),
            jax.ShapeDtypeStruct((turned.shape[0], 2 * HEAD_SIZE), jnp.float32),
        ],
        in_specs=[VMEM] * 4,
        out_specs=[VMEM] * 2,
        compiler_params=LIMIT,
        cost_estimate=pl.CostEstimate(
            flops=12 * work * HEAD_SIZE, bytes_accessed=4 * turned.size, transcendentals=work
        ),
    )(turned, own, beside, above)


def far(turned, own, first_half, second_half, state, rows, passed=None):
    work = turned.shape[0] * 192
    width = turned.shape[0] // rows * HEAD_SIZE
    extra = [] if passed is None else [passed]
    return pl.pallas_call(
        far_kernel,
        out_shape=jax.ShapeDtypeStruct((rows, width * (1 + len(extra))), jnp.bfloat16),
        in_specs=[VMEM] * (6 + len(extra)),
        out_specs=VMEM,
        scratch_shapes=[pltpu.VMEM((2 * first_half.shape[0], own.shape[1]), jnp.bfloat16)],
        compiler_params=LIMIT,
        cost_estimate=pl.CostEstimate(
            flops=12 * work * HEAD_SIZE, bytes_accessed=4 * turned.size, transcendentals=work
        ),
    )(turned, own, first_half, second_half, *state, *extra)


def passed_along(value, axis, steps):
    count = lax.axis_size(axis)
    pairs = [(source, (source + steps) % count) for source in range(count)]
    return lax.ppermute(value, axis, pairs)


def turned_pair(value_entries, cosine, sine):
    half_width = value_entries.shape[-1] // 2
    first = value_entries[..., :half_width].astype(jnp.float32)
    second = value_entries[..., half_width:].astype(jnp.float32)
    cos_wide = cosine[:, None, :]
    sin_wide = sine[:, None, :]
    return jnp.concatenate(
        [first * cos_wide - second * sin_wide, second * cos_wide + first * sin_wide], axis=-1
    )


def attend_head(query_rows, key_rows, value_rows, cache_keys, cache_values, length, block_rows):
    scale = 1.0 / math.sqrt(query_rows.shape[-1])
    contract = (((1,), (1,)), ((), ()))
    cache_live = jnp.arange(cache_keys.shape[0], dtype=jnp.int32) < length
    results = []
    for block_index in range(query_rows.shape[0] // block_rows):
        first_row = block_index * block_rows
        key_reach = first_row + block_rows
        block_queries = query_rows[first_row:key_reach]
        cache_scores = (
            lax.dot_general(block_queries, cache_keys, contract, preferred_element_type=jnp.float32)
            * scale
        )
        own_scores = (
            lax.dot_general(
                block_queries, key_rows[:key_reach], contract, preferred_element_type=jnp.float32
            )
            * scale
        )
        cache_scores = jnp.where(cache_live[None, :], cache_scores, -jnp.inf)
        row_place = first_row + jnp.arange(block_rows, dtype=jnp.int32)
        causal = jnp.arange(key_reach, dtype=jnp.int32)[None, :] <= row_place[:, None]
        own_scores = jnp.where(causal, own_scores, -jnp.inf)
        row_top = jnp.maximum(jnp.max(cache_scores, axis=1), jnp.max(own_scores, axis=1))
        cache_weights = jnp.exp(cache_scores - row_top[:, None])
        own_weights = jnp.exp(own_scores - row_top[:, None])
        row_total = jnp.sum(cache_weights, axis=1) + jnp.sum(own_weights, axis=1)
        numerator = jnp.dot(
            cache_weights.astype(jnp.bfloat16), cache_values, preferred_element_type=jnp.float32
        )
        numerator = numerator + jnp.dot(
            own_weights.astype(jnp.bfloat16),
            value_rows[:key_reach],
            preferred_element_type=jnp.float32,
        )
        results.append((numerator / row_total[:, None]).astype(jnp.bfloat16))
    return jnp.concatenate(results, axis=0)


def head_exchange(query, keyval, cache, offsets, lengths):
    token_row_block = query.shape[1]
    group_total = lax.axis_size("sp")
    local_slots = cache.shape[1]
    head_copies = local_slots * group_total // KEY_VALUE_HEADS
    local_queries = query[0].reshape(token_row_block, QUERY_HEADS, HEAD_SIZE)
    head_queries = lax.all_to_all(local_queries, "sp", split_axis=1, concat_axis=0, tiled=True)
    span_rows = head_queries.shape[0]
    heads_here = head_queries.shape[1]
    local_head_pairs = keyval[0].reshape(token_row_block, KEY_VALUE_HEADS, 2 * HEAD_SIZE)
    broadened = jnp.repeat(local_head_pairs, head_copies, axis=1)
    head_pairs = lax.all_to_all(broadened, "sp", split_axis=1, concat_axis=0, tiled=True)
    positions = offsets[0] + jnp.arange(span_rows, dtype=jnp.int32)
    cosine, sine = rotation_tables(positions, HEAD_SIZE)
    rotated_keys = turned_pair(head_pairs[..., :HEAD_SIZE], cosine, sine).astype(jnp.bfloat16)
    plain_values = head_pairs[..., HEAD_SIZE:]
    section_cache = cache[0]
    length = lengths[0]
    per_slot = heads_here // local_slots
    block_rows = min(512, span_rows)

    def head_step(head_index, finished):
        slot_index = head_index // per_slot
        picked = lax.dynamic_slice_in_dim(head_queries, head_index, 1, 1)
        rotated = turned_pair(picked, cosine, sine)[:, 0].astype(jnp.bfloat16)
        slot_keys = lax.dynamic_index_in_dim(rotated_keys, slot_index, 1, False)
        slot_values = lax.dynamic_index_in_dim(plain_values, slot_index, 1, False)
        slot_cache = lax.dynamic_index_in_dim(section_cache, slot_index, 0, False)
        result = attend_head(
            rotated,
            slot_keys,
            slot_values,
            slot_cache[:, :HEAD_SIZE],
            slot_cache[:, HEAD_SIZE:],
            length,
            block_rows,
        )
        return lax.dynamic_update_slice_in_dim(finished, result[:, None, :], head_index, 1)

    finished = lax.fori_loop(
        0, heads_here, head_step, jnp.zeros((span_rows, heads_here, HEAD_SIZE), jnp.bfloat16)
    )
    passed = passed_along(finished, "section", 1)
    moved = lax.all_to_all(passed, "sp", split_axis=0, concat_axis=1, tiled=True).reshape(
        token_row_block, QUERY_HEADS * HEAD_SIZE
    )
    return moved.reshape(1, token_row_block, QUERY_HEADS * HEAD_SIZE)


def on_device(query, keyval, cache, offsets, lengths):
    rows = query.shape[1]
    chunks = cache.shape[1]
    heads = KEY_VALUE_HEADS // chunks
    positions = offsets[0] + lax.axis_index("sp") * rows + jnp.arange(rows, dtype=jnp.int32)
    cosine, sine = rotation_tables(positions, HEAD_SIZE)
    cosine = jnp.concatenate([cosine, cosine], axis=1)
    sine = jnp.concatenate([-sine, sine], axis=1)
    pack_rows = heads * rows + cache.shape[2] + 16
    half = (pack_rows - 16) // 2
    here, ahead = pl.pallas_call(
        pack_kernel,
        out_shape=[jax.ShapeDtypeStruct((pack_rows, 2 * HEAD_SIZE), jnp.bfloat16)] * chunks,
        in_specs=[VMEM] * 4 + [pl.BlockSpec(memory_space=pltpu.SMEM)],
        out_specs=[VMEM] * chunks,
        compiler_params=LIMIT,
        cost_estimate=pl.CostEstimate(flops=2**30, bytes_accessed=2**21, transcendentals=0),
    )(keyval[0], cache[0], cosine, sine, lengths)
    turned_here, turned_ahead = pl.pallas_call(
        turn_kernel,
        out_shape=[
            jax.ShapeDtypeStruct((query.size // (HEAD_SIZE * chunks), HEAD_SIZE), jnp.bfloat16)
        ]
        * chunks,
        in_specs=[VMEM] * 3,
        out_specs=[VMEM] * chunks,
        compiler_params=LIMIT,
        cost_estimate=pl.CostEstimate(flops=2**30, bytes_accessed=2**23, transcendentals=0),
    )(query[0], cosine, sine)
    beside = partner_swap(here, 1)
    above = partner_swap(here, 2)
    moved_pack = section_shift(ahead)
    moved_query = section_shift(turned_ahead)
    first_half = partner_swap(beside[:half], 2)
    second_half = partner_swap(above[half : 2 * half], 1)
    moved_beside = partner_swap(moved_pack, 1)
    moved_above = partner_swap(moved_pack, 2)
    state = near(turned_here, here, beside, above)
    attended = far(turned_here, here, first_half, second_half, state, rows)
    passed = section_shift(attended)
    moved_first = partner_swap(moved_beside[:half], 2)
    moved_second = partner_swap(moved_above[half : 2 * half], 1)
    state = near(moved_query, moved_pack, moved_beside, moved_above)
    return far(moved_query, moved_pack, moved_first, moved_second, state, rows, passed)[None]


def solution(mesh):
    if mesh.shape["sp"] != 4:
        return jax.shard_map(
            head_exchange, mesh=mesh, in_specs=SPECS, out_specs=SPECS[0], check_vma=False
        )

    return jax.shard_map(
        on_device,
        mesh=mesh,
        in_specs=SPECS,
        out_specs=SPECS[0],
        check_vma=False,
    )
```

```python
import functools
import math

import jax
import jax.numpy as jnp
from jax import lax
from jax.experimental import pallas as pl
from jax.experimental.pallas import tpu as pltpu
from jax.sharding import PartitionSpec as P


QUERY_HEADS = 64
KEY_VALUE_HEADS = 8
HEAD_SIZE = 128
GROUP = QUERY_HEADS // KEY_VALUE_HEADS


ROPE_BASE = 500000.0
MASKED = -1e30
FACTOR = math.log2(math.e) / math.sqrt(HEAD_SIZE)
SPECS = (
    P("section", "sp", None),
    P("section", "sp", None),
    P("section", "sp", None, None),
    P("section"),
    P("section"),
)
VMEM = pl.BlockSpec(memory_space=pltpu.VMEM)
HBM = pl.BlockSpec(memory_space=pltpu.HBM)
LIMIT = pltpu.CompilerParams(vmem_limit_bytes=20 * 2**20)


def section_shift(value, side=None):
    count = lax.axis_size("section")
    pairs = [(i, (i + 1) % count) for i in range(count) if side is None or i % 2 == side]
    return lax.ppermute(value, "section", pairs)


def partner_swap(value, bits):
    count = lax.axis_size("sp")
    return lax.ppermute(value, "sp", [(i, i ^ bits) for i in range(count)])


def rotation_tables(positions, head_width):
    half_width = head_width // 2
    exponent = jnp.arange(half_width, dtype=jnp.float32) * (-2.0 / head_width)
    frequency = jnp.power(jnp.float32(ROPE_BASE), exponent)
    angle = positions.astype(jnp.float32)[:, None] * frequency[None, :]
    return (jnp.cos(angle), jnp.sin(angle))


def rotation_frequency(head_width):
    exponent = jnp.arange(head_width // 2, dtype=jnp.float32) * (-2.0 / head_width)
    frequency = jnp.power(jnp.float32(ROPE_BASE), exponent)
    return jnp.concatenate([frequency, frequency])


def rotated(value, cosine, sine):
    wide = value.astype(jnp.float32)
    turned = pltpu.roll(wide, HEAD_SIZE // 2, 1)
    return (wide * cosine + turned * sine).astype(jnp.bfloat16)


def pack_kernel(
    keyval, cache, offsets, lengths, frequency, *rest
):
    packs, (cosine, sine, loaded, offset, length, sem) = rest[:-6], rest[-6:]
    rows, positions = keyval.shape[0], cache.shape[1]
    heads = KEY_VALUE_HEADS // len(packs)
    middle = heads // 2 * rows
    last = heads * rows + positions
    moves = [(offsets, offset), (lengths, length), (keyval, loaded)]
    for chunk, pack in enumerate(packs):
        moves.append((cache.at[chunk], pack.at[middle : middle + positions]))
    copies = [
        pltpu.make_async_copy(source, target, sem.at[place])
        for place, (source, target) in enumerate(moves)
    ]
    for copy in copies:
        copy.start()
    copies[0].wait()
    first = offset[0] + lax.axis_index("sp") * rows
    place = first + lax.broadcasted_iota(jnp.int32, cosine.shape, 0)
    angle = place.astype(jnp.float32) * frequency[...]
    low = lax.broadcasted_iota(jnp.int32, cosine.shape, 1) < HEAD_SIZE // 2
    cosine[...] = jnp.cos(angle)
    turn = jnp.sin(angle)
    sine[...] = jnp.where(low, -turn, turn)
    for copy in copies[1:]:
        copy.wait()
    cos_here, sin_here = cosine[...], sine[...]
    live = length[0].astype(jnp.float32)
    for chunk, pack in enumerate(packs):
        for index in range(heads):
            start = index * rows + (positions if index >= heads // 2 else 0)
            column = (index * len(packs) + chunk) * 2 * HEAD_SIZE
            pack[start : start + rows, :HEAD_SIZE] = rotated(
                loaded[:, column : column + HEAD_SIZE], cos_here, sin_here
            )
            pack[start : start + rows, HEAD_SIZE:] = loaded[
                :, column + HEAD_SIZE : column + 2 * HEAD_SIZE
            ]
        pack[last:, :] = jnp.full((pack.shape[0] - last, pack.shape[1]), live, jnp.float32).astype(
            jnp.bfloat16
        )


def turn_kernel(query, cosine, sine, *turned):
    rows = query.shape[0]
    cos_here, sin_here = cosine[...], sine[...]
    for head in range(QUERY_HEADS):
        pair = head // GROUP
        chunk, index = pair % len(turned), pair // len(turned)
        start = (index * GROUP + head % GROUP) * rows
        turned[chunk][start : start + rows, :] = rotated(
            query[:, head * HEAD_SIZE : (head + 1) * HEAD_SIZE], cos_here, sin_here
        )


STEP_HEADS = GROUP


def dot_scores(picked, keys):
    return lax.dot_general(
        picked, keys, (((1,), (1,)), ((), ())), preferred_element_type=jnp.float32
    )


def weighted(weights, values):
    values = jnp.concatenate([values, jnp.ones_like(values)], axis=1)
    return jnp.dot(weights, values, preferred_element_type=jnp.float32)


def live_mask(own, positions):
    last = own.shape[0] - 16
    length = own[last : last + 1, :].astype(jnp.float32)
    place = lax.broadcasted_iota(jnp.int32, (1, positions), 1).astype(jnp.float32)
    return place < length[:, :positions]


def run_on_side(body, side, *refs):
    if side is None:
        body(*refs)
    else:
        pl.when(lax.axis_index("section") % 2 == side)(lambda: body(*refs))


def stored_parts(parts):
    keys = jnp.concatenate([part[:, :HEAD_SIZE] for part in parts], axis=0)
    return keys, jnp.concatenate([part[:, HEAD_SIZE:] for part in parts], axis=0)


def near_kernel(rows, side, *refs):
    run_on_side(functools.partial(near_body, rows), side, *refs)


def near_body(rows, query, own, *rest):
    halves, (top_ref, sums_ref, beside, above) = rest[:4], rest[4:]
    me = lax.axis_index("sp")
    heads = query.shape[0] // (GROUP * rows)
    positions = own.shape[0] - 16 - heads * rows
    middle = heads // 2 * rows
    half = halves[0].shape[0]
    for block, first, second in ((beside, *halves[:2]), (above, *halves[2:])):
        block[:half, :] = first[...]
        block[half:, :] = second[: block.shape[0] - half, :]
    blocks = (own, beside, above)
    live = live_mask(own, positions)
    step_rows = STEP_HEADS * rows
    causal = lax.broadcasted_iota(jnp.int32, (rows, rows), 1) <= lax.broadcasted_iota(
        jnp.int32, (rows, rows), 0
    )
    causal = jnp.concatenate([causal] * STEP_HEADS, axis=0)
    for offset in range(len(blocks) + 1):
        head = me ^ offset
        start = pl.multiple_of(head * rows + jnp.where(head >= heads // 2, positions, 0), rows)
        parts = [block[pl.ds(start, rows), :] for block in blocks]
        if offset < len(blocks):
            parts.append(blocks[offset][middle : middle + positions, :])
        keys, values = stored_parts(parts)
        base = pl.multiple_of(head * (GROUP * rows), rows)
        for step in range(GROUP // STEP_HEADS):
            place = pl.ds(base + step * step_rows, step_rows)
            scores = dot_scores(query[place, :], keys)
            pieces = [jnp.where(causal, scores[:, :rows], MASKED)]
            for other in range(1, len(blocks)):
                piece = scores[:, other * rows : (other + 1) * rows]
                pieces.append(jnp.where((me ^ other) < me, piece, MASKED))
            if offset < len(blocks):
                pieces.append(jnp.where(live, scores[:, len(blocks) * rows :], MASKED))
            scores = jnp.concatenate(pieces, axis=1)
            top = jnp.max(scores, axis=1, keepdims=True)
            weights = jnp.exp2((scores - top) * FACTOR).astype(jnp.bfloat16)
            sums_ref[place, :] = weighted(weights, values)
            top_ref[place, :] = jnp.broadcast_to(top, (step_rows, HEAD_SIZE))


def far_kernel(rows, stride, side, *refs):
    run_on_side(functools.partial(far_body, rows, stride), side, *refs)


def far_body(rows, stride, query, own, first_half, second_half, top_ref, sums_ref, *rest):
    out, across, results, sem = rest if len(rest) == 4 else (*rest, None, None)
    me = lax.axis_index("sp")
    heads = query.shape[0] // (GROUP * rows)
    half = first_half.shape[0]
    positions = 2 * half - heads * rows
    middle = heads // 2 * rows
    width = GROUP * HEAD_SIZE
    across[:half, :] = first_half[...]
    across[half:, :] = second_half[: across.shape[0] - half, :]
    live = live_mask(own, positions)
    step_rows = STEP_HEADS * rows
    far = heads - 1
    copies = []
    for offset in range(heads):
        head = me ^ offset
        start = pl.multiple_of(head * rows + jnp.where(head >= heads // 2, positions, 0), rows)
        parts = [across[pl.ds(start, rows), :]]
        if offset == far:
            parts.append(across[middle : middle + positions, :])
        keys, values = stored_parts(parts)
        base = pl.multiple_of(head * (GROUP * rows), rows)
        for step in range(GROUP // STEP_HEADS):
            place = pl.ds(base + step * step_rows, step_rows)
            scores = dot_scores(query[place, :], keys)
            pieces = [jnp.where((me ^ far) < me, scores[:, :rows], MASKED)]
            if offset == far:
                pieces.append(jnp.where(live, scores[:, rows:], MASKED))
            scores = jnp.concatenate(pieces, axis=1)
            before = top_ref[place, :]
            top = jnp.maximum(jnp.max(scores, axis=1, keepdims=True), before)
            kept = jnp.exp2((before - top) * FACTOR)
            wide_top = jnp.concatenate([top] * (scores.shape[1] // HEAD_SIZE), axis=1)
            weights = jnp.exp2((scores - wide_top) * FACTOR).astype(jnp.bfloat16)
            sums = weighted(weights, values) + sums_ref[place, :] * jnp.concatenate(
                [kept, kept], axis=1
            )
            result = (sums[:, :HEAD_SIZE] / sums[:, HEAD_SIZE:]).astype(jnp.bfloat16)
            for part in range(STEP_HEADS):
                lane = (step * STEP_HEADS + part) * HEAD_SIZE
                piece = result[part * rows : (part + 1) * rows]
                if results is None:
                    column = pl.multiple_of(head * width + lane, HEAD_SIZE)
                    out[:, pl.ds(column, HEAD_SIZE)] = piece
                else:
                    results[offset, :, lane : lane + HEAD_SIZE] = piece
        if results is not None:
            column = pl.multiple_of((stride * head + stride - 1) * width, width)
            copy = pltpu.make_async_copy(
                results.at[offset], out.at[:, pl.ds(column, width)], sem.at[offset]
            )
            copy.start()
            copies.append(copy)
    for copy in copies:
        copy.wait()


def join_kernel(from_odd, from_even, before, out, sem):
    width = GROUP * HEAD_SIZE

    def place(passed):
        copies = []
        for index in range(passed.shape[1] // width):
            copies.append(
                pltpu.make_async_copy(
                    passed.at[:, index * width : (index + 1) * width],
                    out.at[:, 2 * index * width : (2 * index + 1) * width],
                    sem.at[index],
                )
            )
        for copy in copies:
            copy.start()
        for copy in copies:
            copy.wait()

    for passed, side in ((from_odd, 0), (from_even, 1)):
        run_on_side(place, side, passed)


def near(turned, rows, own, beside, above, side=None):
    block = pltpu.VMEM((own.shape[0] - 16, own.shape[1]), jnp.bfloat16)
    work = turned.shape[0] * 5 * rows
    return pl.pallas_call(
        functools.partial(near_kernel, rows, side),
        out_shape=[
            pltpu.VMEM((turned.shape[0], HEAD_SIZE), jnp.float32),
            pltpu.VMEM((turned.shape[0], 2 * HEAD_SIZE), jnp.float32),
        ],
        in_specs=[VMEM] * 6,
        out_specs=[VMEM] * 2,
        scratch_shapes=[block] * 2,
        compiler_params=LIMIT,
        cost_estimate=pl.CostEstimate(
            flops=12 * work * HEAD_SIZE, bytes_accessed=4 * turned.size, transcendentals=work
        ),
    )(turned, own, *beside, *above)


def far(turned, rows, own, first_half, second_half, state, stride=1, side=None):
    work = turned.shape[0] * 2 * rows
    width = turned.shape[0] // rows * HEAD_SIZE
    heads = width // (GROUP * HEAD_SIZE)
    scratch = [pltpu.VMEM((2 * first_half.shape[0], 2 * HEAD_SIZE), jnp.bfloat16)]
    if stride > 1:
        scratch.append(pltpu.VMEM((heads, rows, GROUP * HEAD_SIZE), jnp.bfloat16))
        scratch.append(pltpu.SemaphoreType.DMA((heads,)))
    place = pltpu.VMEM if stride == 1 else pltpu.HBM
    return pl.pallas_call(
        functools.partial(far_kernel, rows, stride, side),
        out_shape=place((rows, width * stride), jnp.bfloat16),
        in_specs=[VMEM] * 6,
        out_specs=pl.BlockSpec(memory_space=place),
        scratch_shapes=scratch,
        compiler_params=LIMIT,
        cost_estimate=pl.CostEstimate(
            flops=12 * work * HEAD_SIZE, bytes_accessed=4 * turned.size, transcendentals=work
        ),
    )(turned, own, first_half, second_half, *state)


def passed_along(value, axis, steps):
    count = lax.axis_size(axis)
    pairs = [(source, (source + steps) % count) for source in range(count)]
    return lax.ppermute(value, axis, pairs)


def turned_pair(value_entries, cosine, sine):
    half_width = value_entries.shape[-1] // 2
    first = value_entries[..., :half_width].astype(jnp.float32)
    second = value_entries[..., half_width:].astype(jnp.float32)
    cos_wide = cosine[:, None, :]
    sin_wide = sine[:, None, :]
    return jnp.concatenate(
        [first * cos_wide - second * sin_wide, second * cos_wide + first * sin_wide], axis=-1
    )


def attend_head(query_rows, key_rows, value_rows, cache_keys, cache_values, length, block_rows):
    scale = 1.0 / math.sqrt(query_rows.shape[-1])
    contract = (((1,), (1,)), ((), ()))
    cache_live = jnp.arange(cache_keys.shape[0], dtype=jnp.int32) < length
    results = []
    for block_index in range(query_rows.shape[0] // block_rows):
        first_row = block_index * block_rows
        key_reach = first_row + block_rows
        block_queries = query_rows[first_row:key_reach]
        cache_scores = (
            lax.dot_general(block_queries, cache_keys, contract, preferred_element_type=jnp.float32)
            * scale
        )
        own_scores = (
            lax.dot_general(
                block_queries, key_rows[:key_reach], contract, preferred_element_type=jnp.float32
            )
            * scale
        )
        cache_scores = jnp.where(cache_live[None, :], cache_scores, -jnp.inf)
        row_place = first_row + jnp.arange(block_rows, dtype=jnp.int32)
        causal = jnp.arange(key_reach, dtype=jnp.int32)[None, :] <= row_place[:, None]
        own_scores = jnp.where(causal, own_scores, -jnp.inf)
        row_top = jnp.maximum(jnp.max(cache_scores, axis=1), jnp.max(own_scores, axis=1))
        cache_weights = jnp.exp(cache_scores - row_top[:, None])
        own_weights = jnp.exp(own_scores - row_top[:, None])
        row_total = jnp.sum(cache_weights, axis=1) + jnp.sum(own_weights, axis=1)
        numerator = jnp.dot(
            cache_weights.astype(jnp.bfloat16), cache_values, preferred_element_type=jnp.float32
        )
        numerator = numerator + jnp.dot(
            own_weights.astype(jnp.bfloat16),
            value_rows[:key_reach],
            preferred_element_type=jnp.float32,
        )
        results.append((numerator / row_total[:, None]).astype(jnp.bfloat16))
    return jnp.concatenate(results, axis=0)


def head_exchange(query, keyval, cache, offsets, lengths):
    token_row_block = query.shape[1]
    group_total = lax.axis_size("sp")
    local_slots = cache.shape[1]
    head_copies = local_slots * group_total // KEY_VALUE_HEADS
    local_queries = query[0].reshape(token_row_block, QUERY_HEADS, HEAD_SIZE)
    head_queries = lax.all_to_all(local_queries, "sp", split_axis=1, concat_axis=0, tiled=True)
    span_rows = head_queries.shape[0]
    heads_here = head_queries.shape[1]
    local_head_pairs = keyval[0].reshape(token_row_block, KEY_VALUE_HEADS, 2 * HEAD_SIZE)
    broadened = jnp.repeat(local_head_pairs, head_copies, axis=1)
    head_pairs = lax.all_to_all(broadened, "sp", split_axis=1, concat_axis=0, tiled=True)
    positions = offsets[0] + jnp.arange(span_rows, dtype=jnp.int32)
    cosine, sine = rotation_tables(positions, HEAD_SIZE)
    rotated_keys = turned_pair(head_pairs[..., :HEAD_SIZE], cosine, sine).astype(jnp.bfloat16)
    plain_values = head_pairs[..., HEAD_SIZE:]
    section_cache = cache[0]
    length = lengths[0]
    per_slot = heads_here // local_slots
    block_rows = min(512, span_rows)

    def head_step(head_index, finished):
        slot_index = head_index // per_slot
        picked = lax.dynamic_slice_in_dim(head_queries, head_index, 1, 1)
        rotated = turned_pair(picked, cosine, sine)[:, 0].astype(jnp.bfloat16)
        slot_keys = lax.dynamic_index_in_dim(rotated_keys, slot_index, 1, False)
        slot_values = lax.dynamic_index_in_dim(plain_values, slot_index, 1, False)
        slot_cache = lax.dynamic_index_in_dim(section_cache, slot_index, 0, False)
        result = attend_head(
            rotated,
            slot_keys,
            slot_values,
            slot_cache[:, :HEAD_SIZE],
            slot_cache[:, HEAD_SIZE:],
            length,
            block_rows,
        )
        return lax.dynamic_update_slice_in_dim(finished, result[:, None, :], head_index, 1)

    finished = lax.fori_loop(
        0, heads_here, head_step, jnp.zeros((span_rows, heads_here, HEAD_SIZE), jnp.bfloat16)
    )
    passed = passed_along(finished, "section", 1)
    moved = lax.all_to_all(passed, "sp", split_axis=0, concat_axis=1, tiled=True).reshape(
        token_row_block, QUERY_HEADS * HEAD_SIZE
    )
    return moved.reshape(1, token_row_block, QUERY_HEADS * HEAD_SIZE)


def on_device(query, keyval, cache, offsets, lengths):
    rows = query.shape[1]
    chunks = cache.shape[1]
    heads = KEY_VALUE_HEADS // chunks
    half = (heads * rows + cache.shape[2]) // 2
    pack = pltpu.VMEM((2 * half + 16, 2 * HEAD_SIZE), jnp.bfloat16)
    table = pltpu.VMEM((rows, HEAD_SIZE), jnp.float32)
    items = [pltpu.with_memory_space_constraint(x, pltpu.HBM) for x in (keyval[0], cache[0])]
    items += [offsets, lengths]
    here, ahead, cosine, sine = pl.pallas_call(
        pack_kernel,
        out_shape=[pack] * chunks + [table] * 2,
        in_specs=[HBM] * 4 + [VMEM],
        out_specs=[VMEM] * (chunks + 2),
        scratch_shapes=[
            pltpu.VMEM(keyval.shape[1:], jnp.bfloat16),
            pltpu.SMEM((1,), jnp.int32),
            pltpu.SMEM((1,), jnp.int32),
            pltpu.SemaphoreType.DMA((3 + chunks,)),
        ],
        compiler_params=LIMIT,
        cost_estimate=pl.CostEstimate(flops=2**30, bytes_accessed=2**21, transcendentals=0),
    )(*items, rotation_frequency(HEAD_SIZE)[None])
    turned = pltpu.VMEM((query.size // (HEAD_SIZE * chunks), HEAD_SIZE), jnp.bfloat16)
    turned_here, turned_ahead = pl.pallas_call(
        turn_kernel,
        out_shape=[turned] * chunks,
        in_specs=[VMEM] * 3,
        out_specs=[VMEM] * chunks,
        compiler_params=LIMIT,
        cost_estimate=pl.CostEstimate(flops=2**30, bytes_accessed=2**23, transcendentals=0),
    )(query[0], cosine, sine)
    beside = [partner_swap(here[:half], 1)]
    above = [partner_swap(here[half:], 2)]
    beside.append(partner_swap(here[half:], 1))
    above.insert(0, partner_swap(here[:half], 2))
    moved_pack = section_shift(ahead)
    moved_query = section_shift(turned_ahead)
    first_half = partner_swap(beside[0], 2)
    second_half = partner_swap(above[1], 1)
    moved_beside = [partner_swap(moved_pack[:half], 1)]
    moved_above = [partner_swap(moved_pack[half:], 2)]
    moved_beside.append(partner_swap(moved_pack[half:], 1))
    moved_above.insert(0, partner_swap(moved_pack[:half], 2))
    state = near(turned_here, rows, here, beside, above)
    passed = []
    for side in (1, 0):
        attended = far(turned_here, rows, here, first_half, second_half, state, side=side)
        passed.append(section_shift(attended, side))
    moved_first = partner_swap(moved_beside[0], 2)
    moved_second = partner_swap(moved_above[1], 1)
    state = near(moved_query, rows, moved_pack, moved_beside, moved_above)
    out = far(moved_query, rows, moved_pack, moved_first, moved_second, state, chunks)
    out = pl.pallas_call(
        join_kernel,
        out_shape=pltpu.HBM(out.shape, out.dtype),
        in_specs=[VMEM, VMEM, HBM],
        out_specs=HBM,
        scratch_shapes=[pltpu.SemaphoreType.DMA((heads,))],
        input_output_aliases={2: 0},
        compiler_params=LIMIT,
        cost_estimate=pl.CostEstimate(flops=2**20, bytes_accessed=2**21, transcendentals=0),
    )(*passed, out)
    return out[None]


def solution(mesh):
    if mesh.shape["sp"] != 4:
        return jax.shard_map(
            head_exchange, mesh=mesh, in_specs=SPECS, out_specs=SPECS[0], check_vma=False
        )

    return jax.shard_map(
        on_device,
        mesh=mesh,
        in_specs=SPECS,
        out_specs=SPECS[0],
        check_vma=False,
    )
```

```python
import functools
import math

import jax
import jax.numpy as jnp
from jax import lax
from jax.experimental import pallas as pl
from jax.experimental.pallas import tpu as pltpu
from jax.sharding import PartitionSpec as P


QUERY_HEADS = 64
KEY_VALUE_HEADS = 8
HEAD_SIZE = 128
GROUP = QUERY_HEADS // KEY_VALUE_HEADS


ROPE_BASE = 500000.0
MASKED = -1e30
LENGTH_ROWS = 16
FACTOR = math.log2(math.e) / math.sqrt(HEAD_SIZE)
SPECS = (
    P("section", "sp", None),
    P("section", "sp", None),
    P("section", "sp", None, None),
    P("section"),
    P("section"),
)
VMEM = pl.BlockSpec(memory_space=pltpu.VMEM)
SMEM = pl.BlockSpec(memory_space=pltpu.SMEM)
HBM = pl.BlockSpec(memory_space=pltpu.HBM)
LIMIT = pltpu.CompilerParams(vmem_limit_bytes=20 * 2**20)


def section_shift(value):
    count = lax.axis_size("section")
    return lax.ppermute(value, "section", [(i, (i + 1) % count) for i in range(count)])


def section_swap(value):
    count = lax.axis_size("section")
    return lax.ppermute(value, "section", [(i, i ^ 1) for i in range(count)])


def partner_swap(value, bits):
    count = lax.axis_size("sp")
    return lax.ppermute(value, "sp", [(i, i ^ bits) for i in range(count)])


def rotation_tables(positions, head_width):
    half_width = head_width // 2
    exponent = jnp.arange(half_width, dtype=jnp.float32) * (-2.0 / head_width)
    frequency = jnp.power(jnp.float32(ROPE_BASE), exponent)
    angle = positions.astype(jnp.float32)[:, None] * frequency[None, :]
    return (jnp.cos(angle), jnp.sin(angle))


def rotation_frequency(head_width):
    exponent = jnp.arange(head_width // 2, dtype=jnp.float32) * (-2.0 / head_width)
    frequency = jnp.power(jnp.float32(ROPE_BASE), exponent)
    return jnp.concatenate([frequency, frequency])


def rotated(value, cosine, sine):
    wide = value.astype(jnp.float32)
    turned = pltpu.roll(wide, HEAD_SIZE // 2, 1)
    return (wide * cosine + turned * sine).astype(jnp.bfloat16)


def pack_kernel(keyval, cache, frequency, offset, *rest):
    packs, (cosine, sine, loaded, sem) = rest[:-4], rest[-4:]
    rows, positions = keyval.shape[0], cache.shape[1]
    heads = KEY_VALUE_HEADS // len(packs)
    middle = heads // 2 * rows
    moves = [(keyval, loaded)]
    for chunk, pack in enumerate(packs):
        moves.append((cache.at[chunk], pack.at[middle : middle + positions]))
    copies = [
        pltpu.make_async_copy(source, target, sem.at[place])
        for place, (source, target) in enumerate(moves)
    ]
    for copy in copies:
        copy.start()
    first = offset[0] + lax.axis_index("sp") * rows
    place = first + lax.broadcasted_iota(jnp.int32, cosine.shape, 0)
    angle = place.astype(jnp.float32) * frequency[...]
    low = lax.broadcasted_iota(jnp.int32, cosine.shape, 1) < HEAD_SIZE // 2
    cosine[...] = jnp.cos(angle)
    turn = jnp.sin(angle)
    sine[...] = jnp.where(low, -turn, turn)
    copies[0].wait()
    cos_here, sin_here = cosine[...], sine[...]
    for chunk, pack in enumerate(packs):
        for index in range(heads):
            start = index * rows + (positions if index >= heads // 2 else 0)
            column = (index * len(packs) + chunk) * 2 * HEAD_SIZE
            pack[start : start + rows, :HEAD_SIZE] = rotated(
                loaded[:, column : column + HEAD_SIZE], cos_here, sin_here
            )
            pack[start : start + rows, HEAD_SIZE:] = loaded[
                :, column + HEAD_SIZE : column + 2 * HEAD_SIZE
            ]
    for copy in copies[1:]:
        copy.wait()


def turn_kernel(query, cosine, sine, length, *turned):
    rows = query.shape[0]
    cos_here, sin_here = cosine[...], sine[...]
    live = length[0].astype(jnp.float32)
    for part in turned:
        part[part.shape[0] - LENGTH_ROWS :, :] = jnp.full(
            (LENGTH_ROWS, HEAD_SIZE), live, jnp.float32
        ).astype(jnp.bfloat16)
    for head in range(QUERY_HEADS):
        pair = head // GROUP
        chunk, index = pair % len(turned), pair // len(turned)
        start = (index * GROUP + head % GROUP) * rows
        turned[chunk][start : start + rows, :] = rotated(
            query[:, head * HEAD_SIZE : (head + 1) * HEAD_SIZE], cos_here, sin_here
        )


STEP_HEADS = GROUP


def dot_scores(picked, keys):
    return lax.dot_general(
        picked, keys, (((1,), (1,)), ((), ())), preferred_element_type=jnp.float32
    )


def weighted(weights, values):
    values = jnp.concatenate([values, jnp.ones_like(values)], axis=1)
    return jnp.dot(weights, values, preferred_element_type=jnp.float32)


def own_heads(query, rows):
    return (query.shape[0] - LENGTH_ROWS) // (GROUP * rows)


def live_mask(query, positions):
    last = query.shape[0] - LENGTH_ROWS
    length = query[last : last + 1, :].astype(jnp.float32)
    length = jnp.concatenate([length] * (positions // HEAD_SIZE), axis=1)
    place = lax.broadcasted_iota(jnp.int32, (1, positions), 1).astype(jnp.float32)
    return place < length


def run_on_side(body, side, *refs):
    if side is None:
        body(*refs)
    else:
        pl.when(lax.axis_index("section") % 2 == side)(lambda: body(*refs))


def stored_parts(parts):
    keys = jnp.concatenate([part[:, :HEAD_SIZE] for part in parts], axis=0)
    return keys, jnp.concatenate([part[:, HEAD_SIZE:] for part in parts], axis=0)


def near_kernel(rows, side, *refs):
    run_on_side(functools.partial(near_body, rows), side, *refs)


def near_body(rows, query, own, *rest):
    halves, (top_ref, sums_ref, beside, above) = rest[:4], rest[4:]
    me = lax.axis_index("sp")
    heads = own_heads(query, rows)
    positions = own.shape[0] - heads * rows
    middle = heads // 2 * rows
    half = halves[0].shape[0]
    for block, first, second in ((beside, *halves[:2]), (above, *halves[2:])):
        block[:half, :] = first[...]
        block[half:, :] = second[...]
    blocks = (own, beside, above)
    live = live_mask(query, positions)
    step_rows = STEP_HEADS * rows
    for offset in range(len(blocks) + 1):
        head = me ^ offset
        start = pl.multiple_of(head * rows + jnp.where(head >= heads // 2, positions, 0), rows)
        parts = [block[pl.ds(start, rows), :] for block in blocks[1:]]
        if offset < len(blocks):
            parts.append(blocks[offset][middle : middle + positions, :])
        keys, values = stored_parts(parts)
        base = pl.multiple_of(head * (GROUP * rows), rows)
        for step in range(GROUP // STEP_HEADS):
            place = pl.ds(base + step * step_rows, step_rows)
            scores = dot_scores(query[place, :], keys)
            pieces = []
            for other in range(1, len(blocks)):
                piece = scores[:, (other - 1) * rows : other * rows]
                pieces.append(jnp.where((me ^ other) < me, piece, MASKED))
            if offset < len(blocks):
                pieces.append(jnp.where(live, scores[:, (len(blocks) - 1) * rows :], MASKED))
            scores = jnp.concatenate(pieces, axis=1)
            top = jnp.max(scores, axis=1, keepdims=True)
            weights = jnp.exp2((scores - top) * FACTOR).astype(jnp.bfloat16)
            sums_ref[place, :] = weighted(weights, values)
            top_ref[place, :] = jnp.broadcast_to(top, (step_rows, HEAD_SIZE))


def far_kernel(rows, stride, side, *refs):
    run_on_side(functools.partial(far_body, rows, stride), side, *refs)


def far_body(rows, stride, query, own, first_half, second_half, top_ref, sums_ref, *rest):
    out, across, results, sem = rest if len(rest) == 4 else (*rest, None, None)
    me = lax.axis_index("sp")
    heads = own_heads(query, rows)
    half = first_half.shape[0]
    positions = 2 * half - heads * rows
    middle = heads // 2 * rows
    width = GROUP * HEAD_SIZE
    across[:half, :] = first_half[...]
    across[half:, :] = second_half[...]
    live = live_mask(query, positions)
    step_rows = STEP_HEADS * rows
    causal = lax.broadcasted_iota(jnp.int32, (rows, rows), 1) <= lax.broadcasted_iota(
        jnp.int32, (rows, rows), 0
    )
    causal = jnp.concatenate([causal] * STEP_HEADS, axis=0)
    far = heads - 1
    copies = []
    for offset in range(heads):
        head = me ^ offset
        start = pl.multiple_of(head * rows + jnp.where(head >= heads // 2, positions, 0), rows)
        parts = [own[pl.ds(start, rows), :], across[pl.ds(start, rows), :]]
        if offset == far:
            parts.append(across[middle : middle + positions, :])
        keys, values = stored_parts(parts)
        base = pl.multiple_of(head * (GROUP * rows), rows)
        for step in range(GROUP // STEP_HEADS):
            place = pl.ds(base + step * step_rows, step_rows)
            scores = dot_scores(query[place, :], keys)
            pieces = [
                jnp.where(causal, scores[:, :rows], MASKED),
                jnp.where((me ^ far) < me, scores[:, rows : 2 * rows], MASKED),
            ]
            if offset == far:
                pieces.append(jnp.where(live, scores[:, 2 * rows :], MASKED))
            scores = jnp.concatenate(pieces, axis=1)
            before = top_ref[place, :]
            top = jnp.maximum(jnp.max(scores, axis=1, keepdims=True), before)
            kept = jnp.exp2((before - top) * FACTOR)
            wide_top = jnp.concatenate([top] * (scores.shape[1] // HEAD_SIZE), axis=1)
            weights = jnp.exp2((scores - wide_top) * FACTOR).astype(jnp.bfloat16)
            sums = weighted(weights, values) + sums_ref[place, :] * jnp.concatenate(
                [kept, kept], axis=1
            )
            result = (sums[:, :HEAD_SIZE] / sums[:, HEAD_SIZE:]).astype(jnp.bfloat16)
            for part in range(STEP_HEADS):
                lane = (step * STEP_HEADS + part) * HEAD_SIZE
                piece = result[part * rows : (part + 1) * rows]
                if results is None:
                    column = pl.multiple_of(head * width + lane, HEAD_SIZE)
                    out[:, pl.ds(column, HEAD_SIZE)] = piece
                else:
                    results[offset, :, lane : lane + HEAD_SIZE] = piece
        if results is not None:
            column = pl.multiple_of((stride * head + stride - 1) * width, width)
            copy = pltpu.make_async_copy(
                results.at[offset], out.at[:, pl.ds(column, width)], sem.at[offset]
            )
            copy.start()
            copies.append(copy)
    for copy in copies:
        copy.wait()


def join_kernel(from_odd, from_even, before, out, sem):
    width = GROUP * HEAD_SIZE

    def place(passed):
        copies = []
        for index in range(passed.shape[1] // width):
            copies.append(
                pltpu.make_async_copy(
                    passed.at[:, index * width : (index + 1) * width],
                    out.at[:, 2 * index * width : (2 * index + 1) * width],
                    sem.at[index],
                )
            )
        for copy in copies:
            copy.start()
        for copy in copies:
            copy.wait()

    for passed, side in ((from_odd, 0), (from_even, 1)):
        run_on_side(place, side, passed)


def near(turned, rows, own, beside, above, side=None):
    block = pltpu.VMEM(own.shape, jnp.bfloat16)
    work = turned.shape[0] * 5 * rows
    return pl.pallas_call(
        functools.partial(near_kernel, rows, side),
        out_shape=[
            pltpu.VMEM((turned.shape[0] - LENGTH_ROWS, HEAD_SIZE), jnp.float32),
            pltpu.VMEM((turned.shape[0] - LENGTH_ROWS, 2 * HEAD_SIZE), jnp.float32),
        ],
        in_specs=[VMEM] * 6,
        out_specs=[VMEM] * 2,
        scratch_shapes=[block] * 2,
        compiler_params=LIMIT,
        cost_estimate=pl.CostEstimate(
            flops=12 * work * HEAD_SIZE, bytes_accessed=4 * turned.size, transcendentals=work
        ),
    )(turned, own, *beside, *above)


def far(turned, rows, own, first_half, second_half, state, stride=1, side=None):
    work = turned.shape[0] * 2 * rows
    width = (turned.shape[0] - LENGTH_ROWS) // rows * HEAD_SIZE
    heads = width // (GROUP * HEAD_SIZE)
    scratch = [pltpu.VMEM((2 * first_half.shape[0], 2 * HEAD_SIZE), jnp.bfloat16)]
    if stride > 1:
        scratch.append(pltpu.VMEM((heads, rows, GROUP * HEAD_SIZE), jnp.bfloat16))
        scratch.append(pltpu.SemaphoreType.DMA((heads,)))
    place = pltpu.VMEM if stride == 1 else pltpu.HBM
    return pl.pallas_call(
        functools.partial(far_kernel, rows, stride, side),
        out_shape=place((rows, width * stride), jnp.bfloat16),
        in_specs=[VMEM] * 6,
        out_specs=pl.BlockSpec(memory_space=place),
        scratch_shapes=scratch,
        compiler_params=LIMIT,
        cost_estimate=pl.CostEstimate(
            flops=12 * work * HEAD_SIZE, bytes_accessed=4 * turned.size, transcendentals=work
        ),
    )(turned, own, first_half, second_half, *state)


def passed_along(value, axis, steps):
    count = lax.axis_size(axis)
    pairs = [(source, (source + steps) % count) for source in range(count)]
    return lax.ppermute(value, axis, pairs)


def turned_pair(value_entries, cosine, sine):
    half_width = value_entries.shape[-1] // 2
    first = value_entries[..., :half_width].astype(jnp.float32)
    second = value_entries[..., half_width:].astype(jnp.float32)
    cos_wide = cosine[:, None, :]
    sin_wide = sine[:, None, :]
    return jnp.concatenate(
        [first * cos_wide - second * sin_wide, second * cos_wide + first * sin_wide], axis=-1
    )


def attend_head(query_rows, key_rows, value_rows, cache_keys, cache_values, length, block_rows):
    scale = 1.0 / math.sqrt(query_rows.shape[-1])
    contract = (((1,), (1,)), ((), ()))
    cache_live = jnp.arange(cache_keys.shape[0], dtype=jnp.int32) < length
    results = []
    for block_index in range(query_rows.shape[0] // block_rows):
        first_row = block_index * block_rows
        key_reach = first_row + block_rows
        block_queries = query_rows[first_row:key_reach]
        cache_scores = (
            lax.dot_general(block_queries, cache_keys, contract, preferred_element_type=jnp.float32)
            * scale
        )
        own_scores = (
            lax.dot_general(
                block_queries, key_rows[:key_reach], contract, preferred_element_type=jnp.float32
            )
            * scale
        )
        cache_scores = jnp.where(cache_live[None, :], cache_scores, -jnp.inf)
        row_place = first_row + jnp.arange(block_rows, dtype=jnp.int32)
        causal = jnp.arange(key_reach, dtype=jnp.int32)[None, :] <= row_place[:, None]
        own_scores = jnp.where(causal, own_scores, -jnp.inf)
        row_top = jnp.maximum(jnp.max(cache_scores, axis=1), jnp.max(own_scores, axis=1))
        cache_weights = jnp.exp(cache_scores - row_top[:, None])
        own_weights = jnp.exp(own_scores - row_top[:, None])
        row_total = jnp.sum(cache_weights, axis=1) + jnp.sum(own_weights, axis=1)
        numerator = jnp.dot(
            cache_weights.astype(jnp.bfloat16), cache_values, preferred_element_type=jnp.float32
        )
        numerator = numerator + jnp.dot(
            own_weights.astype(jnp.bfloat16),
            value_rows[:key_reach],
            preferred_element_type=jnp.float32,
        )
        results.append((numerator / row_total[:, None]).astype(jnp.bfloat16))
    return jnp.concatenate(results, axis=0)


def head_exchange(query, keyval, cache, offsets, lengths):
    token_row_block = query.shape[1]
    group_total = lax.axis_size("sp")
    local_slots = cache.shape[1]
    head_copies = local_slots * group_total // KEY_VALUE_HEADS
    local_queries = query[0].reshape(token_row_block, QUERY_HEADS, HEAD_SIZE)
    head_queries = lax.all_to_all(local_queries, "sp", split_axis=1, concat_axis=0, tiled=True)
    span_rows = head_queries.shape[0]
    heads_here = head_queries.shape[1]
    local_head_pairs = keyval[0].reshape(token_row_block, KEY_VALUE_HEADS, 2 * HEAD_SIZE)
    broadened = jnp.repeat(local_head_pairs, head_copies, axis=1)
    head_pairs = lax.all_to_all(broadened, "sp", split_axis=1, concat_axis=0, tiled=True)
    positions = offsets[0] + jnp.arange(span_rows, dtype=jnp.int32)
    cosine, sine = rotation_tables(positions, HEAD_SIZE)
    rotated_keys = turned_pair(head_pairs[..., :HEAD_SIZE], cosine, sine).astype(jnp.bfloat16)
    plain_values = head_pairs[..., HEAD_SIZE:]
    section_cache = cache[0]
    length = lengths[0]
    per_slot = heads_here // local_slots
    block_rows = min(512, span_rows)

    def head_step(head_index, finished):
        slot_index = head_index // per_slot
        picked = lax.dynamic_slice_in_dim(head_queries, head_index, 1, 1)
        rotated = turned_pair(picked, cosine, sine)[:, 0].astype(jnp.bfloat16)
        slot_keys = lax.dynamic_index_in_dim(rotated_keys, slot_index, 1, False)
        slot_values = lax.dynamic_index_in_dim(plain_values, slot_index, 1, False)
        slot_cache = lax.dynamic_index_in_dim(section_cache, slot_index, 0, False)
        result = attend_head(
            rotated,
            slot_keys,
            slot_values,
            slot_cache[:, :HEAD_SIZE],
            slot_cache[:, HEAD_SIZE:],
            length,
            block_rows,
        )
        return lax.dynamic_update_slice_in_dim(finished, result[:, None, :], head_index, 1)

    finished = lax.fori_loop(
        0, heads_here, head_step, jnp.zeros((span_rows, heads_here, HEAD_SIZE), jnp.bfloat16)
    )
    passed = passed_along(finished, "section", 1)
    moved = lax.all_to_all(passed, "sp", split_axis=0, concat_axis=1, tiled=True).reshape(
        token_row_block, QUERY_HEADS * HEAD_SIZE
    )
    return moved.reshape(1, token_row_block, QUERY_HEADS * HEAD_SIZE)


def on_device(query, keyval, cache, offsets, lengths):
    rows = query.shape[1]
    chunks = cache.shape[1]
    heads = KEY_VALUE_HEADS // chunks
    half = (heads * rows + cache.shape[2]) // 2
    pack = pltpu.VMEM((2 * half, 2 * HEAD_SIZE), jnp.bfloat16)
    table = pltpu.VMEM((rows, HEAD_SIZE), jnp.float32)
    items = [pltpu.with_memory_space_constraint(x, pltpu.HBM) for x in (keyval[0], cache[0])]
    here, ahead, cosine, sine = pl.pallas_call(
        pack_kernel,
        out_shape=[pack] * chunks + [table] * 2,
        in_specs=[HBM] * 2 + [VMEM, SMEM],
        out_specs=[VMEM] * (chunks + 2),
        scratch_shapes=[
            pltpu.VMEM(keyval.shape[1:], jnp.bfloat16),
            pltpu.SemaphoreType.DMA((1 + chunks,)),
        ],
        compiler_params=LIMIT,
        cost_estimate=pl.CostEstimate(flops=2**30, bytes_accessed=2**21, transcendentals=0),
    )(*items, rotation_frequency(HEAD_SIZE)[None], offsets)
    lengths, cosine = lax.optimization_barrier((lengths, cosine))
    turned_rows = query.size // (HEAD_SIZE * chunks) + LENGTH_ROWS
    turned = pltpu.VMEM((turned_rows, HEAD_SIZE), jnp.bfloat16)
    turned_here, turned_ahead = pl.pallas_call(
        turn_kernel,
        out_shape=[turned] * chunks,
        in_specs=[VMEM] * 3 + [SMEM],
        out_specs=[VMEM] * chunks,
        compiler_params=LIMIT,
        cost_estimate=pl.CostEstimate(flops=2**30, bytes_accessed=2**23, transcendentals=0),
    )(query[0], cosine, sine, lengths)
    beside = [partner_swap(here[:half], 1)]
    above = [partner_swap(here[half:], 2)]
    beside.append(partner_swap(here[half:], 1))
    above.insert(0, partner_swap(here[:half], 2))
    moved_pack = section_shift(ahead)
    moved_query = section_shift(turned_ahead)
    first_half = partner_swap(beside[0], 2)
    second_half = partner_swap(above[1], 1)
    moved_beside = [partner_swap(moved_pack[:half], 1)]
    moved_above = [partner_swap(moved_pack[half:], 2)]
    moved_beside.append(partner_swap(moved_pack[half:], 1))
    moved_above.insert(0, partner_swap(moved_pack[:half], 2))
    state = near(turned_here, rows, here, beside, above)
    attended = far(turned_here, rows, here, first_half, second_half, state, side=1)
    from_odd = section_shift(attended)
    attended = far(turned_here, rows, here, first_half, second_half, state, side=0)
    from_even = section_swap(attended)
    moved_first = partner_swap(moved_beside[0], 2)
    moved_second = partner_swap(moved_above[1], 1)
    state = near(moved_query, rows, moved_pack, moved_beside, moved_above)
    out = far(moved_query, rows, moved_pack, moved_first, moved_second, state, chunks)
    out = pl.pallas_call(
        join_kernel,
        out_shape=pltpu.HBM(out.shape, out.dtype),
        in_specs=[VMEM, VMEM, HBM],
        out_specs=HBM,
        scratch_shapes=[pltpu.SemaphoreType.DMA((heads,))],
        input_output_aliases={2: 0},
        compiler_params=LIMIT,
        cost_estimate=pl.CostEstimate(flops=2**20, bytes_accessed=2**21, transcendentals=0),
    )(from_odd, from_even, out)
    return out[None]


def solution(mesh):
    if mesh.shape["sp"] != 4:
        return jax.shard_map(
            head_exchange, mesh=mesh, in_specs=SPECS, out_specs=SPECS[0], check_vma=False
        )

    return jax.shard_map(
        on_device,
        mesh=mesh,
        in_specs=SPECS,
        out_specs=SPECS[0],
        check_vma=False,
    )
```

```python
import functools
import math

import jax
import jax.numpy as jnp
from jax import lax
from jax.experimental import pallas as pl
from jax.experimental.pallas import tpu as pltpu
from jax.sharding import PartitionSpec as P


QUERY_HEADS = 64
KEY_VALUE_HEADS = 8
HEAD_SIZE = 128
GROUP = QUERY_HEADS // KEY_VALUE_HEADS


ROPE_BASE = 500000.0
MASKED = -1e30
LENGTH_ROWS = 16
FACTOR = math.log2(math.e) / math.sqrt(HEAD_SIZE)
SPECS = (
    P("section", "sp", None),
    P("section", "sp", None),
    P("section", "sp", None, None),
    P("section"),
    P("section"),
)
VMEM = pl.BlockSpec(memory_space=pltpu.VMEM)
SMEM = pl.BlockSpec(memory_space=pltpu.SMEM)
HBM = pl.BlockSpec(memory_space=pltpu.HBM)
LIMIT = pltpu.CompilerParams(vmem_limit_bytes=20 * 2**20)


def section_shift(value):
    count = lax.axis_size("section")
    return lax.ppermute(value, "section", [(i, (i + 1) % count) for i in range(count)])


def section_swap(value):
    count = lax.axis_size("section")
    return lax.ppermute(value, "section", [(i, i ^ 1) for i in range(count)])


def partner_swap(value, bits):
    count = lax.axis_size("sp")
    return lax.ppermute(value, "sp", [(i, i ^ bits) for i in range(count)])


def rotation_tables(positions, head_width):
    half_width = head_width // 2
    exponent = jnp.arange(half_width, dtype=jnp.float32) * (-2.0 / head_width)
    frequency = jnp.power(jnp.float32(ROPE_BASE), exponent)
    angle = positions.astype(jnp.float32)[:, None] * frequency[None, :]
    return (jnp.cos(angle), jnp.sin(angle))


def rotation_frequency(head_width):
    exponent = jnp.arange(head_width // 2, dtype=jnp.float32) * (-2.0 / head_width)
    frequency = jnp.power(jnp.float32(ROPE_BASE), exponent)
    return jnp.concatenate([frequency, frequency])


def rotated(value, cosine, sine):
    wide = value.astype(jnp.float32)
    turned = pltpu.roll(wide, HEAD_SIZE // 2, 1)
    return (wide * cosine + turned * sine).astype(jnp.bfloat16)


def pack_kernel(keyval, cache, frequency, offset, *rest):
    packs, (cosine, sine, loaded, sem) = rest[:-4], rest[-4:]
    rows, positions = keyval.shape[0], cache.shape[1]
    heads = KEY_VALUE_HEADS // len(packs)
    middle = heads // 2 * rows
    moves = [(keyval, loaded)]
    for chunk, pack in enumerate(packs):
        moves.append((cache.at[chunk], pack.at[middle : middle + positions]))
    copies = [
        pltpu.make_async_copy(source, target, sem.at[place])
        for place, (source, target) in enumerate(moves)
    ]
    for copy in copies:
        copy.start()
    first = offset[0] + lax.axis_index("sp") * rows
    place = first + lax.broadcasted_iota(jnp.int32, cosine.shape, 0)
    angle = place.astype(jnp.float32) * frequency[...]
    low = lax.broadcasted_iota(jnp.int32, cosine.shape, 1) < HEAD_SIZE // 2
    cosine[...] = jnp.cos(angle)
    turn = jnp.sin(angle)
    sine[...] = jnp.where(low, -turn, turn)
    copies[0].wait()
    cos_here, sin_here = cosine[...], sine[...]
    for chunk, pack in enumerate(packs):
        for index in range(heads):
            start = index * rows + (positions if index >= heads // 2 else 0)
            column = (index * len(packs) + chunk) * 2 * HEAD_SIZE
            pack[start : start + rows, :HEAD_SIZE] = rotated(
                loaded[:, column : column + HEAD_SIZE], cos_here, sin_here
            )
            pack[start : start + rows, HEAD_SIZE:] = loaded[
                :, column + HEAD_SIZE : column + 2 * HEAD_SIZE
            ]
    for copy in copies[1:]:
        copy.wait()


def turn_kernel(query, cosine, sine, length, *turned):
    rows = query.shape[0]
    cos_here, sin_here = cosine[...], sine[...]
    live = length[0].astype(jnp.float32)
    for part in turned:
        part[part.shape[0] - LENGTH_ROWS :, :] = jnp.full(
            (LENGTH_ROWS, HEAD_SIZE), live, jnp.float32
        ).astype(jnp.bfloat16)
    for head in range(QUERY_HEADS):
        pair = head // GROUP
        chunk, index = pair % len(turned), pair // len(turned)
        start = (index * GROUP + head % GROUP) * rows
        turned[chunk][start : start + rows, :] = rotated(
            query[:, head * HEAD_SIZE : (head + 1) * HEAD_SIZE], cos_here, sin_here
        )


STEP_HEADS = GROUP


def dot_scores(picked, keys):
    return lax.dot_general(
        picked, keys, (((1,), (1,)), ((), ())), preferred_element_type=jnp.float32
    )


def weighted(weights, values):
    values = jnp.concatenate([values, jnp.ones_like(values)], axis=1)
    return jnp.dot(weights, values, preferred_element_type=jnp.float32)


def own_heads(query, rows):
    return (query.shape[0] - LENGTH_ROWS) // (GROUP * rows)


def live_mask(query, positions):
    last = query.shape[0] - LENGTH_ROWS
    length = query[last : last + 1, :].astype(jnp.float32)
    length = jnp.concatenate([length] * (positions // HEAD_SIZE), axis=1)
    place = lax.broadcasted_iota(jnp.int32, (1, positions), 1).astype(jnp.float32)
    return place < length


def causal_mask(rows):
    causal = lax.broadcasted_iota(jnp.int32, (rows, rows), 1) <= lax.broadcasted_iota(
        jnp.int32, (rows, rows), 0
    )
    return jnp.concatenate([causal] * STEP_HEADS, axis=0)


def run_on_side(body, side, *refs):
    if side is None:
        body(*refs)
    else:
        pl.when(lax.axis_index("section") % 2 == side)(lambda: body(*refs))


def stored_parts(parts):
    keys = jnp.concatenate([part[:, :HEAD_SIZE] for part in parts], axis=0)
    return keys, jnp.concatenate([part[:, HEAD_SIZE:] for part in parts], axis=0)


def near_kernel(rows, own_sides, *refs):
    if len(own_sides) == 2:
        near_body(rows, True, *refs)
    else:
        for side in (0, 1):
            run_on_side(functools.partial(near_body, rows, side in own_sides), side, *refs)


def near_body(rows, with_own, query, own, *rest):
    halves, (top_ref, sums_ref, beside, above) = rest[:4], rest[4:]
    me = lax.axis_index("sp")
    heads = own_heads(query, rows)
    positions = own.shape[0] - heads * rows
    middle = heads // 2 * rows
    half = halves[0].shape[0]
    for block, first, second in ((beside, *halves[:2]), (above, *halves[2:])):
        block[:half, :] = first[...]
        block[half:, :] = second[...]
    blocks = (own, beside, above)
    live = live_mask(query, positions)
    step_rows = STEP_HEADS * rows
    causal = causal_mask(rows)
    for offset in range(len(blocks) + 1):
        head = me ^ offset
        start = pl.multiple_of(head * rows + jnp.where(head >= heads // 2, positions, 0), rows)
        near_blocks = blocks if with_own else blocks[1:]
        parts = [block[pl.ds(start, rows), :] for block in near_blocks]
        if offset < len(blocks):
            parts.append(blocks[offset][middle : middle + positions, :])
        keys, values = stored_parts(parts)
        base = pl.multiple_of(head * (GROUP * rows), rows)
        for step in range(GROUP // STEP_HEADS):
            place = pl.ds(base + step * step_rows, step_rows)
            scores = dot_scores(query[place, :], keys)
            pieces = []
            if with_own:
                pieces.append(jnp.where(causal, scores[:, :rows], MASKED))
            for other in range(1, len(blocks)):
                left = len(pieces) * rows
                piece = scores[:, left : left + rows]
                pieces.append(jnp.where((me ^ other) < me, piece, MASKED))
            if offset < len(blocks):
                pieces.append(jnp.where(live, scores[:, len(pieces) * rows :], MASKED))
            scores = jnp.concatenate(pieces, axis=1)
            top = jnp.max(scores, axis=1, keepdims=True)
            weights = jnp.exp2((scores - top) * FACTOR).astype(jnp.bfloat16)
            sums_ref[place, :] = weighted(weights, values)
            top_ref[place, :] = jnp.broadcast_to(top, (step_rows, HEAD_SIZE))


def far_kernel(rows, stride, with_own, side, *refs):
    run_on_side(functools.partial(far_body, rows, stride, with_own), side, *refs)


def far_body(rows, stride, with_own, query, own, first_half, second_half, top_ref, sums_ref, *rest):
    out, across, results, sem = rest if len(rest) == 4 else (*rest, None, None)
    me = lax.axis_index("sp")
    heads = own_heads(query, rows)
    half = first_half.shape[0]
    positions = 2 * half - heads * rows
    middle = heads // 2 * rows
    width = GROUP * HEAD_SIZE
    across[:half, :] = first_half[...]
    across[half:, :] = second_half[...]
    live = live_mask(query, positions)
    step_rows = STEP_HEADS * rows
    causal = causal_mask(rows)
    far = heads - 1
    copies = []
    for offset in range(heads):
        head = me ^ offset
        start = pl.multiple_of(head * rows + jnp.where(head >= heads // 2, positions, 0), rows)
        far_blocks = (own, across) if with_own else (across,)
        parts = [block[pl.ds(start, rows), :] for block in far_blocks]
        if offset == far:
            parts.append(across[middle : middle + positions, :])
        keys, values = stored_parts(parts)
        base = pl.multiple_of(head * (GROUP * rows), rows)
        for step in range(GROUP // STEP_HEADS):
            place = pl.ds(base + step * step_rows, step_rows)
            scores = dot_scores(query[place, :], keys)
            pieces = []
            if with_own:
                pieces.append(jnp.where(causal, scores[:, :rows], MASKED))
            left = len(pieces) * rows
            pieces.append(jnp.where((me ^ far) < me, scores[:, left : left + rows], MASKED))
            if offset == far:
                pieces.append(jnp.where(live, scores[:, left + rows :], MASKED))
            scores = jnp.concatenate(pieces, axis=1)
            before = top_ref[place, :]
            top = jnp.maximum(jnp.max(scores, axis=1, keepdims=True), before)
            kept = jnp.exp2((before - top) * FACTOR)
            wide_top = jnp.concatenate([top] * (scores.shape[1] // HEAD_SIZE), axis=1)
            weights = jnp.exp2((scores - wide_top) * FACTOR).astype(jnp.bfloat16)
            sums = weighted(weights, values) + sums_ref[place, :] * jnp.concatenate(
                [kept, kept], axis=1
            )
            result = (sums[:, :HEAD_SIZE] / sums[:, HEAD_SIZE:]).astype(jnp.bfloat16)
            for part in range(STEP_HEADS):
                lane = (step * STEP_HEADS + part) * HEAD_SIZE
                piece = result[part * rows : (part + 1) * rows]
                if results is None:
                    column = pl.multiple_of(head * width + lane, HEAD_SIZE)
                    out[:, pl.ds(column, HEAD_SIZE)] = piece
                else:
                    results[offset, :, lane : lane + HEAD_SIZE] = piece
        if results is not None:
            column = pl.multiple_of((stride * head + stride - 1) * width, width)
            copy = pltpu.make_async_copy(
                results.at[offset], out.at[:, pl.ds(column, width)], sem.at[offset]
            )
            copy.start()
            copies.append(copy)
    for copy in copies:
        copy.wait()


def join_kernel(from_odd, from_even, before, out, sem):
    width = GROUP * HEAD_SIZE

    def place(passed):
        copies = []
        for index in range(passed.shape[1] // width):
            copies.append(
                pltpu.make_async_copy(
                    passed.at[:, index * width : (index + 1) * width],
                    out.at[:, 2 * index * width : (2 * index + 1) * width],
                    sem.at[index],
                )
            )
        for copy in copies:
            copy.start()
        for copy in copies:
            copy.wait()

    for passed, side in ((from_odd, 0), (from_even, 1)):
        run_on_side(place, side, passed)


def near(turned, rows, own, beside, above, own_sides):
    block = pltpu.VMEM(own.shape, jnp.bfloat16)
    work = turned.shape[0] * 5 * rows
    return pl.pallas_call(
        functools.partial(near_kernel, rows, own_sides),
        out_shape=[
            pltpu.VMEM((turned.shape[0] - LENGTH_ROWS, HEAD_SIZE), jnp.float32),
            pltpu.VMEM((turned.shape[0] - LENGTH_ROWS, 2 * HEAD_SIZE), jnp.float32),
        ],
        in_specs=[VMEM] * 6,
        out_specs=[VMEM] * 2,
        scratch_shapes=[block] * 2,
        compiler_params=LIMIT,
        cost_estimate=pl.CostEstimate(
            flops=12 * work * HEAD_SIZE, bytes_accessed=4 * turned.size, transcendentals=work
        ),
    )(turned, own, *beside, *above)


def far(turned, rows, own, first_half, second_half, state, with_own, stride=1, side=None):
    work = turned.shape[0] * 2 * rows
    width = (turned.shape[0] - LENGTH_ROWS) // rows * HEAD_SIZE
    heads = width // (GROUP * HEAD_SIZE)
    scratch = [pltpu.VMEM((2 * first_half.shape[0], 2 * HEAD_SIZE), jnp.bfloat16)]
    if stride > 1:
        scratch.append(pltpu.VMEM((heads, rows, GROUP * HEAD_SIZE), jnp.bfloat16))
        scratch.append(pltpu.SemaphoreType.DMA((heads,)))
    place = pltpu.VMEM if stride == 1 else pltpu.HBM
    return pl.pallas_call(
        functools.partial(far_kernel, rows, stride, with_own, side),
        out_shape=place((rows, width * stride), jnp.bfloat16),
        in_specs=[VMEM] * 6,
        out_specs=pl.BlockSpec(memory_space=place),
        scratch_shapes=scratch,
        compiler_params=LIMIT,
        cost_estimate=pl.CostEstimate(
            flops=12 * work * HEAD_SIZE, bytes_accessed=4 * turned.size, transcendentals=work
        ),
    )(turned, own, first_half, second_half, *state)


def passed_along(value, axis, steps):
    count = lax.axis_size(axis)
    pairs = [(source, (source + steps) % count) for source in range(count)]
    return lax.ppermute(value, axis, pairs)


def turned_pair(value_entries, cosine, sine):
    half_width = value_entries.shape[-1] // 2
    first = value_entries[..., :half_width].astype(jnp.float32)
    second = value_entries[..., half_width:].astype(jnp.float32)
    cos_wide = cosine[:, None, :]
    sin_wide = sine[:, None, :]
    return jnp.concatenate(
        [first * cos_wide - second * sin_wide, second * cos_wide + first * sin_wide], axis=-1
    )


def attend_head(query_rows, key_rows, value_rows, cache_keys, cache_values, length, block_rows):
    scale = 1.0 / math.sqrt(query_rows.shape[-1])
    contract = (((1,), (1,)), ((), ()))
    cache_live = jnp.arange(cache_keys.shape[0], dtype=jnp.int32) < length
    results = []
    for block_index in range(query_rows.shape[0] // block_rows):
        first_row = block_index * block_rows
        key_reach = first_row + block_rows
        block_queries = query_rows[first_row:key_reach]
        cache_scores = (
            lax.dot_general(block_queries, cache_keys, contract, preferred_element_type=jnp.float32)
            * scale
        )
        own_scores = (
            lax.dot_general(
                block_queries, key_rows[:key_reach], contract, preferred_element_type=jnp.float32
            )
            * scale
        )
        cache_scores = jnp.where(cache_live[None, :], cache_scores, -jnp.inf)
        row_place = first_row + jnp.arange(block_rows, dtype=jnp.int32)
        causal = jnp.arange(key_reach, dtype=jnp.int32)[None, :] <= row_place[:, None]
        own_scores = jnp.where(causal, own_scores, -jnp.inf)
        row_top = jnp.maximum(jnp.max(cache_scores, axis=1), jnp.max(own_scores, axis=1))
        cache_weights = jnp.exp(cache_scores - row_top[:, None])
        own_weights = jnp.exp(own_scores - row_top[:, None])
        row_total = jnp.sum(cache_weights, axis=1) + jnp.sum(own_weights, axis=1)
        numerator = jnp.dot(
            cache_weights.astype(jnp.bfloat16), cache_values, preferred_element_type=jnp.float32
        )
        numerator = numerator + jnp.dot(
            own_weights.astype(jnp.bfloat16),
            value_rows[:key_reach],
            preferred_element_type=jnp.float32,
        )
        results.append((numerator / row_total[:, None]).astype(jnp.bfloat16))
    return jnp.concatenate(results, axis=0)


def head_exchange(query, keyval, cache, offsets, lengths):
    token_row_block = query.shape[1]
    group_total = lax.axis_size("sp")
    local_slots = cache.shape[1]
    head_copies = local_slots * group_total // KEY_VALUE_HEADS
    local_queries = query[0].reshape(token_row_block, QUERY_HEADS, HEAD_SIZE)
    head_queries = lax.all_to_all(local_queries, "sp", split_axis=1, concat_axis=0, tiled=True)
    span_rows = head_queries.shape[0]
    heads_here = head_queries.shape[1]
    local_head_pairs = keyval[0].reshape(token_row_block, KEY_VALUE_HEADS, 2 * HEAD_SIZE)
    broadened = jnp.repeat(local_head_pairs, head_copies, axis=1)
    head_pairs = lax.all_to_all(broadened, "sp", split_axis=1, concat_axis=0, tiled=True)
    positions = offsets[0] + jnp.arange(span_rows, dtype=jnp.int32)
    cosine, sine = rotation_tables(positions, HEAD_SIZE)
    rotated_keys = turned_pair(head_pairs[..., :HEAD_SIZE], cosine, sine).astype(jnp.bfloat16)
    plain_values = head_pairs[..., HEAD_SIZE:]
    section_cache = cache[0]
    length = lengths[0]
    per_slot = heads_here // local_slots
    block_rows = min(512, span_rows)

    def head_step(head_index, finished):
        slot_index = head_index // per_slot
        picked = lax.dynamic_slice_in_dim(head_queries, head_index, 1, 1)
        rotated = turned_pair(picked, cosine, sine)[:, 0].astype(jnp.bfloat16)
        slot_keys = lax.dynamic_index_in_dim(rotated_keys, slot_index, 1, False)
        slot_values = lax.dynamic_index_in_dim(plain_values, slot_index, 1, False)
        slot_cache = lax.dynamic_index_in_dim(section_cache, slot_index, 0, False)
        result = attend_head(
            rotated,
            slot_keys,
            slot_values,
            slot_cache[:, :HEAD_SIZE],
            slot_cache[:, HEAD_SIZE:],
            length,
            block_rows,
        )
        return lax.dynamic_update_slice_in_dim(finished, result[:, None, :], head_index, 1)

    finished = lax.fori_loop(
        0, heads_here, head_step, jnp.zeros((span_rows, heads_here, HEAD_SIZE), jnp.bfloat16)
    )
    passed = passed_along(finished, "section", 1)
    moved = lax.all_to_all(passed, "sp", split_axis=0, concat_axis=1, tiled=True).reshape(
        token_row_block, QUERY_HEADS * HEAD_SIZE
    )
    return moved.reshape(1, token_row_block, QUERY_HEADS * HEAD_SIZE)


def on_device(query, keyval, cache, offsets, lengths):
    rows = query.shape[1]
    chunks = cache.shape[1]
    heads = KEY_VALUE_HEADS // chunks
    half = (heads * rows + cache.shape[2]) // 2
    pack = pltpu.VMEM((2 * half, 2 * HEAD_SIZE), jnp.bfloat16)
    table = pltpu.VMEM((rows, HEAD_SIZE), jnp.float32)
    items = [pltpu.with_memory_space_constraint(x, pltpu.HBM) for x in (keyval[0], cache[0])]
    here, ahead, cosine, sine = pl.pallas_call(
        pack_kernel,
        out_shape=[pack] * chunks + [table] * 2,
        in_specs=[HBM] * 2 + [VMEM, SMEM],
        out_specs=[VMEM] * (chunks + 2),
        scratch_shapes=[
            pltpu.VMEM(keyval.shape[1:], jnp.bfloat16),
            pltpu.SemaphoreType.DMA((1 + chunks,)),
        ],
        compiler_params=LIMIT,
        cost_estimate=pl.CostEstimate(flops=2**30, bytes_accessed=2**21, transcendentals=0),
    )(*items, rotation_frequency(HEAD_SIZE)[None], offsets)
    lengths, cosine = lax.optimization_barrier((lengths, cosine))
    turned_rows = query.size // (HEAD_SIZE * chunks) + LENGTH_ROWS
    turned = pltpu.VMEM((turned_rows, HEAD_SIZE), jnp.bfloat16)
    turned_here, turned_ahead = pl.pallas_call(
        turn_kernel,
        out_shape=[turned] * chunks,
        in_specs=[VMEM] * 3 + [SMEM],
        out_specs=[VMEM] * chunks,
        compiler_params=LIMIT,
        cost_estimate=pl.CostEstimate(flops=2**30, bytes_accessed=2**23, transcendentals=0),
    )(query[0], cosine, sine, lengths)
    beside = [partner_swap(here[:half], 1)]
    above = [partner_swap(here[half:], 2)]
    beside.append(partner_swap(here[half:], 1))
    above.insert(0, partner_swap(here[:half], 2))
    moved_pack = section_shift(ahead)
    moved_query = section_shift(turned_ahead)
    first_half = partner_swap(beside[0], 2)
    second_half = partner_swap(above[1], 1)
    moved_beside = [partner_swap(moved_pack[:half], 1)]
    moved_above = [partner_swap(moved_pack[half:], 2)]
    moved_beside.append(partner_swap(moved_pack[half:], 1))
    moved_above.insert(0, partner_swap(moved_pack[:half], 2))
    state = near(turned_here, rows, here, beside, above, (1,))
    attended = far(turned_here, rows, here, first_half, second_half, state, False, side=1)
    from_odd = section_shift(attended)
    attended = far(turned_here, rows, here, first_half, second_half, state, True, side=0)
    from_even = section_swap(attended)
    moved_first = partner_swap(moved_beside[0], 2)
    moved_second = partner_swap(moved_above[1], 1)
    state = near(moved_query, rows, moved_pack, moved_beside, moved_above, (0, 1))
    out = far(moved_query, rows, moved_pack, moved_first, moved_second, state, False, chunks)
    out = pl.pallas_call(
        join_kernel,
        out_shape=pltpu.HBM(out.shape, out.dtype),
        in_specs=[VMEM, VMEM, HBM],
        out_specs=HBM,
        scratch_shapes=[pltpu.SemaphoreType.DMA((heads,))],
        input_output_aliases={2: 0},
        compiler_params=LIMIT,
        cost_estimate=pl.CostEstimate(flops=2**20, bytes_accessed=2**21, transcendentals=0),
    )(from_odd, from_even, out)
    return out[None]


def solution(mesh):
    if mesh.shape["sp"] != 4:
        return jax.shard_map(
            head_exchange, mesh=mesh, in_specs=SPECS, out_specs=SPECS[0], check_vma=False
        )

    return jax.shard_map(
        on_device,
        mesh=mesh,
        in_specs=SPECS,
        out_specs=SPECS[0],
        check_vma=False,
    )
```
